32 devices in a mesh: seq: 4 (over z), blk: 4 (over y, core), uly: 2 (over x).
Axes of the slice: x: 2, y: 2, z: 4, core: 2. Of those that a mesh axis runs over, the one named last changes fastest.
Arguments:
- queries: bfloat16 [8192, 5120], P(('seq', 'blk', 'uly')), parts along dimension 0, may hold values from -60 to 60, as said below
- keys: bfloat16 [8192, 1024], P(('seq', 'blk', 'uly')), parts along dimension 0, may hold values from -60 to 60, as said below
- values: bfloat16 [8192, 1024], P(('seq', 'blk', 'uly')), parts along dimension 0, may hold values from -6 to 6
- positions: int32 [3, 8192], P(None, ('seq', 'blk', 'uly')), parts along dimension 1, may hold values from 0 to 526
- doc_lengths: int32 [32], P('seq'), parts along dimension 0, may hold values from 1 to 1024, 2048 in all
Outputs:
- attended: bfloat16 [8192, 5120], P(('seq', 'blk', 'uly')), parts along dimension 0
The draws below stay inside these ranges and needn't reach their ends.
There are 4 independent parts, one for each index of `seq`. The reference program is written for one: setup_inputs(seed, part) draws one part's arguments, and reference() takes and returns one part's arrays. A program takes and returns all parts, laid end to end along the dimension named above; each array names one. Nothing has to cross between parts.
Inputs may be any that keep to these rules, and one draw needn't show every extreme that they name: queries; the query rows hold values of order one, a few rows may be much larger. keys; the key rows hold values of order one, a few rows may be much larger.
All inputs are finite; a program needn't handle non-finite values.
Results may differ from the reference program's by a relative error of at most 0.0055.
Values may be sent and summed in bfloat16 or wider, within the bound.
A program may use at most 384 MiB of HBM per device.

```python
import math
import jax
import jax.numpy as jnp
import numpy as np
from jax import lax

KEY_VALUE_HEADS = 8
HEAD_SIZE = 128
QUERY_PER_KEY = 5
HQ = 40
NDOC = 8
PACKED_TOKENS = 2048


def draw_queries(key, part):
    frequency_base = jnp.clip(jax.random.normal(jax.random.fold_in(key, 1), (PACKED_TOKENS, HQ * HEAD_SIZE), jnp.float32), -6.0, 6.0)
    return frequency_base.astype(jnp.bfloat16)


def draw_keys(key, part):
    frequency_base = jnp.clip(jax.random.normal(jax.random.fold_in(key, 2), (PACKED_TOKENS, KEY_VALUE_HEADS * HEAD_SIZE), jnp.float32), -6.0, 6.0)
    return frequency_base.astype(jnp.bfloat16)


def draw_positions(key, part):
    index = jnp.arange(PACKED_TOKENS, dtype=jnp.int32)
    jitter = jax.random.randint(key, (3, PACKED_TOKENS), 0, 16)
    return (index[None, :] // 4 + jitter).astype(jnp.int32)


def shard_levels(own_key, shape, pieces, least, high):
    def one(axis_at, blocks):
        steps = jax.random.uniform(jax.random.fold_in(jax.random.fold_in(own_key, 6), axis_at), (blocks,), jnp.float32, least / len(pieces), high / len(pieces))
        return jnp.repeat(jnp.exp(steps), shape[axis_at] // blocks).reshape((-1,) + (1,) * (len(shape) - axis_at - 1))

    level = one(*pieces[0])
    for cut in pieces[1:]:
        level = level * one(*cut)
    return level


def profile(count, total, limit, lean):
    loads = [(1 << 20) // math.isqrt(standing ** lean) + 1 for standing in range(2, count + 1)]
    surplus, holding = total - limit - (count - 1), [1] * (count - 1)
    while surplus > 0:
        candidates = [i for i in range(count - 1) if holding[i] < limit]
        mass, remaining = sum([loads[i] for i in candidates]), surplus
        for i in candidates:
            more = min(limit - holding[i], max(1, remaining * loads[i] // mass), surplus)
            holding[i] = holding[i] + more
            surplus = surplus - more
    return np.array([limit] + holding)


def ragged(key, count, total, most, slope):
    if count == 2:
        one = jax.random.randint(key, (), max(1, total - most), min(most, total - 1) + 1)
        return jnp.stack([one, total - one])
    sizes = jnp.asarray(profile(count, total, most, slope), jnp.int32)
    pairs = (count - 1) // 2
    donor, sink = sizes[1:1 + 2 * pairs:2], sizes[2:2 + 2 * pairs:2]
    margin = jnp.minimum(donor - 1, most - sink)
    passed = jax.random.randint(jax.random.fold_in(key, 1), (pairs,), 0, 1 << 20) % (margin + 1)
    sizes = sizes.at[1:1 + 2 * pairs:2].set(donor - passed).at[2:2 + 2 * pairs:2].set(sink + passed)
    return sizes[jax.random.permutation(jax.random.fold_in(key, 2), count)]


def normal_values(own_key, shape, width, bound, shards=(), held_as=jnp.bfloat16):
    factor_of = shard_levels(own_key, shape, shards, -0.22, 0.18) if shards else 1.0
    values = jax.random.normal(own_key, shape, jnp.float32) * width * factor_of
    return jnp.minimum(jnp.maximum(values, -bound), bound).astype(held_as)


def setup_inputs(seed: int = 0, part: int = 0) -> dict:
    key_list = jax.random.split(jax.random.key(seed), 6)
    own_keys = jax.random.split(jax.random.fold_in(key_list[5], part), 6)
    return {
        "queries": draw_queries(jax.random.fold_in(jax.random.fold_in(key_list[5], part), 71), part),
        "keys": draw_keys(jax.random.fold_in(jax.random.fold_in(key_list[5], part), 71), part),
        "values": normal_values(own_keys[2], (PACKED_TOKENS, KEY_VALUE_HEADS * HEAD_SIZE), 1.0, 6.0, ((0, 8),)),
        "positions": draw_positions(jax.random.fold_in(jax.random.fold_in(key_list[5], part), 71), part),
        "doc_lengths": ragged(own_keys[4], NDOC, PACKED_TOKENS, PACKED_TOKENS // 2, 2).astype(jnp.int32),
    }


def apply_rotary(x, pos, heads):
    rows = x.shape[0]
    half = HEAD_SIZE // 2
    pair = jnp.arange(half, dtype=jnp.int32)
    freq = jnp.power(jnp.float32(1000000.0), -2.0 * pair.astype(jnp.float32) / HEAD_SIZE)
    place = pos.astype(jnp.float32)
    first = HEAD_SIZE // 8
    second = first + 3 * HEAD_SIZE // 16
    chosen = jnp.where(pair[None, :] < first, place[0][:, None], jnp.where(pair[None, :] < second, place[1][:, None], place[2][:, None]))
    angle = chosen * freq[None, :]
    cosine = jnp.cos(angle)[:, None, :]
    sine = jnp.sin(angle)[:, None, :]
    parts = x.reshape(rows, heads, HEAD_SIZE).astype(jnp.float32)
    lower = parts[..., :half]
    upper = parts[..., half:]
    turned = jnp.concatenate([lower * cosine - upper * sine, upper * cosine + lower * sine], axis=-1)
    return turned.reshape(rows, heads * HEAD_SIZE).astype(jnp.bfloat16)

def doc_starts(index, doc_lengths):
    ends = jnp.cumsum(doc_lengths).astype(jnp.int32)
    return lax.optimization_barrier(jnp.sum(jnp.where(ends[None, :] <= index[:, None], doc_lengths[None, :], 0), axis=1)).astype(jnp.int32)

def reference(queries, keys, values, positions, doc_lengths):
    query_rotated = apply_rotary(queries, positions, HQ)
    key_rotated = apply_rotary(keys, positions, KEY_VALUE_HEADS)
    index = jnp.arange(PACKED_TOKENS, dtype=jnp.int32)
    starts = doc_starts(index, doc_lengths)
    allowed = (index[None, :] <= index[:, None]) & (index[None, :] >= starts[:, None])
    scale = 1.0 / math.sqrt(HEAD_SIZE)
    grouped_query = jnp.transpose(query_rotated.reshape(PACKED_TOKENS, KEY_VALUE_HEADS, QUERY_PER_KEY, HEAD_SIZE), (1, 0, 2, 3))
    key_heads_view = jnp.transpose(key_rotated.reshape(PACKED_TOKENS, KEY_VALUE_HEADS, HEAD_SIZE), (1, 0, 2))
    value_heads_view = jnp.transpose(values.reshape(PACKED_TOKENS, KEY_VALUE_HEADS, HEAD_SIZE), (1, 0, 2))

    def one_head(operands):
        q_head, k_head, v_head = operands
        scores = jnp.einsum('rgd,bd->grb', q_head.astype(jnp.float32), k_head.astype(jnp.float32)) * scale
        scores = jnp.where(allowed[None], scores, -1e+30)
        best = lax.optimization_barrier(jnp.max(scores, axis=-1, keepdims=True))
        weights = jnp.where(allowed[None], jnp.exp(scores - best), 0.0)
        total = lax.optimization_barrier(jnp.sum(weights, axis=-1))
        weight_b = weights.astype(jnp.bfloat16)
        summed = jnp.einsum('grb,bd->grd', weight_b.astype(jnp.float32), v_head.astype(jnp.float32))
        return summed / total[..., None]
    result = lax.map(one_head, (grouped_query, key_heads_view, value_heads_view))
    return jnp.transpose(result, (2, 0, 1, 3)).reshape(PACKED_TOKENS, HQ * HEAD_SIZE).astype(jnp.bfloat16)
```

```python
import functools
import math

import jax
import jax.numpy as jnp
import numpy as np
from jax import lax
from jax.experimental import pallas as pl
from jax.experimental.pallas import tpu as pltpu
from jax.sharding import PartitionSpec as P

HEAD_SIZE = 128
QUERY_PER_KEY = 5
BURST = 8
SETTLED = 5
FAR = -1e30
SUBLANES = 8


TABLE = {
    "own": {
        1: (8, 4, 2, 0, 8, 8, 2, 0),
        2: (5, 8, 0, 0, 5, 5, 0, 0),
        4: (8, 8, 6, 3, 0, 0, 0, 0),
    },
    "relay": {
        4: ((0, 0, 0, 0, 0, 6, 2, 2), (0, 0, 0, 0, 0, 1, 0, 0)),
        3: ((0, 0, 0, 0, 0, 0, 1, 0), (0, 0, 0, 0, 0, 0, 2, 0)),
        1: ((0, 0, 0, 0, 0, 2, 0, 0), (0, 1, 0, 1, 0, 1, 0, 0)),
    },
    "first": (1, 2, 3, 3, 3, 4, 2, 2),
}


def frequencies():
    pair = np.arange(HEAD_SIZE // 2)
    value = np.power(1000000.0, -2.0 * pair / HEAD_SIZE).astype(np.float32)
    return np.repeat(value[:, None], HEAD_SIZE, axis=1)


def rotary_tables(places, freq):
    rows = places.shape[1]
    half = HEAD_SIZE // 2
    pair = lax.broadcasted_iota(jnp.int32, (half, rows), 0)
    first = HEAD_SIZE // 8
    second = first + 3 * HEAD_SIZE // 16
    place = places.astype(jnp.float32)
    chosen = jnp.where(pair < first, place[0:1], jnp.where(pair < second, place[1:2], place[2:3]))
    angle = chosen * jnp.concatenate([freq] * (rows // HEAD_SIZE), axis=1)
    turns = jnp.floor(angle * (2.0 / math.pi) + 0.5)
    rest = angle - turns * 1.5703125
    rest = rest - turns * 4.8351287841796875e-4
    rest = rest - turns * 3.138552419841289520264e-7
    rest = rest - turns * 6.07710050630396597660e-11
    quarter = turns.astype(jnp.int32) & 3
    square = rest * rest
    sine = rest + rest * square * (
        -1.0 / 6 + square * (1.0 / 120 + square * (-1.0 / 5040 + square * (1.0 / 362880)))
    )
    cosine = 1.0 + square * (
        -0.5 + square * (1.0 / 24 + square * (-1.0 / 720 + square * (1.0 / 40320)))
    )
    swap = (quarter & 1) == 1
    sin_turned = jnp.where(swap, cosine, sine)
    cos_turned = jnp.where(swap, sine, cosine)
    sin_turned = jnp.where(quarter >= 2, -sin_turned, sin_turned)
    cos_turned = jnp.where((quarter == 1) | (quarter == 2), -cos_turned, cos_turned)
    return cos_turned, sin_turned


def routes(blocks, lanes):
    count = blocks * lanes
    window = count // 2

    def place(r):
        return (r // lanes // 2, r % lanes), r // lanes % 2

    def member(chip, core):
        return (chip[0] * 2 + core) * lanes + chip[1]

    found = {}
    for s in range(count):
        home, own_core = place(s)
        wanting = set(range(s + 1, min(count, s + window + 1)))

        def entry(chip):
            if chip == home:
                return s
            for core in (own_core, 1 - own_core):
                if member(chip, core) in wanting:
                    return member(chip, core)
            return None

        for half in (0, 1):
            for r in sorted(wanting):
                chip, _ = place(r)
                source = entry(chip)
                if source == r:
                    options = []
                    if chip[1] != home[1]:
                        options.append(entry((chip[0], home[1])))
                    if chip[0] > home[0]:
                        options.append(entry((chip[0] - 1, chip[1])))
                    if half:
                        options.reverse()
                    options = [o for o in options if o is not None] + [s]
                    source = options[0]
                found.setdefault((source - s, r - source), (set(), set()))[half].add(source)
    return sorted(found.items(), key=lambda item: (-item[0][0], item[0][1]))


def pick(me, values):
    found = jnp.int32(values[0])
    for device, value in enumerate(values):
        if value != values[0]:
            found = jnp.where(me == device, jnp.int32(value), found)
    return found


def timetable(blocks, lanes, window):
    if (blocks, lanes) == (4, 2):
        return TABLE
    return {
        "own": {step: (3,) for step in range(1, blocks * lanes)},
        "relay": {slot: ((0,), (0,)) for slot in range(1, window + 1)},
        "first": (0,),
    }


def among(me, devices):
    hit = jnp.bool_(False)
    for device in sorted(devices):
        hit = hit | (me == device)
    return hit


def kernel(
    plan, lanes, count, window, kheads,
    lengths, places_in, freq_in, keys_in, values_in, queries, out,
    places, freq, keys, values, cosine, sine, cosine_t, sine_t, kv, kfeat, qfeat, tri, qbuf, qt, scores, *rest,
):
    best, held = rest[:QUERY_PER_KEY], rest[QUERY_PER_KEY : 2 * QUERY_PER_KEY]
    q_sem, in_sem, send_sem, recv_sem = rest[2 * QUERY_PER_KEY :]
    rows = keys.shape[0]
    size = HEAD_SIZE
    group = QUERY_PER_KEY * size
    me = lax.axis_index("blk") * lanes + lax.axis_index("uly")

    def where_is(r):
        return {"blk": lax.div(r, lanes), "uly": lax.rem(r, lanes)}

    barrier = pltpu.get_barrier_semaphore()
    for offset in range(1, count):
        peer = lax.rem(me + offset, count)
        pl.semaphore_signal(
            barrier, inc=1, device_id=where_is(peer), device_id_type=pl.DeviceIdType.MESH
        )
    loads = [
        pltpu.make_async_copy(source, target, in_sem.at[i])
        for i, (source, target) in enumerate(
            ((places_in, places), (freq_in, freq), (keys_in, keys), (values_in, values))
        )
    ]
    for load in loads:
        load.start()
    fetch = pltpu.make_async_copy(queries, qbuf, q_sem)
    fetch.start()

    def column(h, width):
        return pl.ds(pl.multiple_of(h * width, width), width)

    loads[0].wait()
    loads[1].wait()
    cos_half, sin_half = rotary_tables(places[...], freq[...])
    cosine_t[...] = cos_half
    sine_t[...] = sin_half
    cosine[...] = jnp.concatenate([cos_half, cos_half], axis=0).T
    sine[...] = jnp.concatenate([-sin_half, sin_half], axis=0).T

    def turn(x):
        x = x.astype(jnp.float32)
        return (x * cosine[...] + pltpu.roll(x, size // 2, 1) * sine[...]).astype(jnp.bfloat16)

    loads[2].wait()
    loads[3].wait()

    def own_block(h, carry):
        kv[0, h, :rows, :] = turn(keys[:, column(h, size)])
        turned = values[:, column(h, size)].astype(jnp.float32).T.astype(jnp.bfloat16)
        for piece in range(rows // size):
            at = rows + piece * size
            kv[0, h, at : at + size, :] = turned[:, piece * size : (piece + 1) * size]
        return carry

    lax.fori_loop(0, kheads, own_block, 0)
    pl.semaphore_wait(barrier, count - 1)

    def copy_of(index, slot, step, h):
        return pltpu.make_async_remote_copy(
            src_ref=kv.at[slot, h],
            dst_ref=kv.at[slot + step, h],
            send_sem=send_sem.at[index, h],
            recv_sem=recv_sem.at[slot + step, h],
            device_id=where_is(me + step),
            device_id_type=pl.DeviceIdType.MESH,
        )

    def arrival(slot, h):
        return pltpu.make_async_remote_copy(
            src_ref=kv.at[slot, h],
            dst_ref=kv.at[slot, h],
            send_sem=send_sem.at[0, h],
            recv_sem=recv_sem.at[slot, h],
            device_id=where_is(me),
            device_id_type=pl.DeviceIdType.MESH,
        )

    def sends(senders, h):
        low, high = senders
        if low == high:
            return among(me, low)
        is_low = h * 2 < kheads
        return (is_low & among(me, low)) | (jnp.logical_not(is_low) & among(me, high))

    table = timetable(count // lanes, lanes, window)

    def relays(slot, h):
        hit = jnp.bool_(False)
        for (from_slot, _), senders in plan:
            if from_slot == slot:
                hit = hit | sends(senders, h)
        return hit

    def send_own(turn_at):
        for index, ((slot, step), senders) in enumerate(plan):
            if slot == 0:
                h = turn_at + pick(me, table["own"][step])

                @pl.when((h >= 0) & (h < kheads) & sends(senders, h))
                def _():
                    copy_of(index, slot, step, h).start()

    def pass_on(turn_at, place):
        for slot in sorted({slot for (slot, _), _ in plan if slot}, reverse=True):
            lead, at = table["relay"][slot]
            if place in at:
                h = turn_at + pick(me, lead)
                now = (h >= 0) & (h < kheads) & relays(slot, h)

                @pl.when(now & (pick(me, at) == place))
                def _():
                    arrival(slot, h).wait_recv()
                    for index, ((from_slot, step), senders) in enumerate(plan):
                        if from_slot == slot:
                            @pl.when(sends(senders, h))
                            def _():
                                copy_of(index, slot, step, h).start()

    def opening(i, carry):
        turn_at = i - BURST
        send_own(turn_at)
        for place in range(3):
            pass_on(turn_at, place)
        return carry

    lax.fori_loop(0, BURST - SETTLED, opening, 0)

    for slot in range(1, window + 1):
        @pl.when(me < slot)
        def _():
            def clear(h, carry):
                kv[slot, h] = jnp.zeros((rows + rows // size * size, size), kv.dtype)
                return carry

            lax.fori_loop(0, kheads, clear, 0)

    lane = lax.broadcasted_iota(jnp.int32, (1, size), 1)
    opens = jnp.zeros((1, size), jnp.int32)
    closes = jnp.zeros((1, size), jnp.int32)
    end = jnp.int32(0)
    for d in range(lengths.shape[0]):
        start, end = end, end + lengths[d]
        opens = jnp.where(lane == d, start, opens)
        closes = jnp.where(lane == d, end, closes)
    row = lax.broadcasted_iota(jnp.int32, (rows, size), 0)
    for slot in range(window + 1):
        token = row + (me - slot) * rows
        inside = (token >= opens) & (token < closes)
        kfeat[slot] = jnp.where(inside, 0.0, FAR).astype(jnp.bfloat16)
        if slot == 0:
            qfeat[...] = jnp.where(inside, 1.0, 0.0).T.astype(jnp.bfloat16)
    key_at = lax.broadcasted_iota(jnp.int32, (rows, rows), 0)
    query_at = lax.broadcasted_iota(jnp.int32, (rows, rows), 1)
    tri[...] = jnp.where(key_at <= query_at, 1.0, 0.0).astype(jnp.bfloat16)

    fetch.wait()

    def turn_queries(h, carry):
        x = qbuf[:, column(h, size)].astype(jnp.float32).T
        low, high = x[: size // 2], x[size // 2 :]
        cos_half, sin_half = cosine_t[...], sine_t[...]
        turned = jnp.concatenate(
            [low * cos_half - high * sin_half, high * cos_half + low * sin_half], axis=0
        )
        qt[h] = turned.astype(jnp.bfloat16)
        return carry

    lax.fori_loop(0, kheads * QUERY_PER_KEY, turn_queries, 0, unroll=QUERY_PER_KEY)

    scale = math.log2(math.e) / math.sqrt(size)
    ones = jnp.ones((2 * SUBLANES, rows), jnp.bfloat16)

    def key_of(slot, h):
        return jnp.concatenate([kv[slot, h, :rows, :], kfeat[slot]], axis=1)

    def value_of(slot, h):
        pieces = [
            kv[slot, h, rows + p * size : rows + (p + 1) * size, :] for p in range(rows // size)
        ]
        return jnp.concatenate([jnp.concatenate(pieces, axis=1), ones], axis=0)

    def query_of(h, g):
        return jnp.concatenate([qt[h * QUERY_PER_KEY + g], qfeat[...]], axis=0)

    def dot(a, b):
        return jnp.dot(a, b, preferred_element_type=jnp.float32)

    def begin(h):
        scores = []
        for g in range(QUERY_PER_KEY):
            q = query_of(h, g)
            scores.append(
                jnp.where(key_at <= query_at, dot(key_of(0, h), q), dot(key_of(window, h), q))
            )
        pending = None
        for g in range(QUERY_PER_KEY + 1):
            if g < QUERY_PER_KEY:
                top = jnp.max(scores[g], axis=0, keepdims=True)
                w = jnp.exp2((scores[g] - top) * scale).astype(jnp.bfloat16)
                near = w * tri[...]
                best[g][h] = jnp.broadcast_to(top, (SUBLANES, rows))
                both = dot(value_of(0, h), near) + dot(value_of(window, h), w - near)
            if pending is not None:
                held[g - 1][h] = pending[: size + SUBLANES]
            pending = both

    def complete(h):
        def score(g):
            q = query_of(h, g)
            top = best[g][h][:1]
            for slot in range(1, window):
                s = dot(key_of(slot, h), q)
                scores[g % 2, slot - 1] = s
                top = jnp.maximum(top, jnp.max(s, axis=0, keepdims=True))
            return top

        def attend(g, top):
            keep = jnp.exp2((best[g][h][:1] - top) * scale)
            both = None
            for slot in range(1, window):
                w = jnp.exp2((scores[g % 2, slot - 1] - top) * scale).astype(jnp.bfloat16)
                part = dot(value_of(slot, h), w)
                both = part if both is None else both + part
            both = both[: size + SUBLANES] + held[g][h] * keep
            settle(h, g, both)

        top = score(0)
        for g in range(QUERY_PER_KEY):
            following = score(g + 1) if g + 1 < QUERY_PER_KEY else None
            attend(g, top)
            top = following

    def settle(h, g, both):
        result = both[:size] * (1.0 / both[size : size + 1])
        at = pl.ds(pl.multiple_of(h * group + g * size, size), size)
        out[:, at] = result.T.astype(jnp.bfloat16)

    def take(slot, h):
        @pl.when((me >= slot) & jnp.logical_not(relays(slot, h)))
        def _():
            arrival(slot, h).wait_recv()

    def rounds(i, carry):
        turn_at = i - SETTLED
        send_own(turn_at)
        pass_on(turn_at, 0)
        first = turn_at + pick(me, table["first"])

        @pl.when((first >= 0) & (first < kheads))
        def _():
            take(window, first)
            begin(first)

        pass_on(turn_at, 1)

        @pl.when(turn_at >= 0)
        def _():
            for slot in range(1, window):
                take(slot, turn_at)

            @pl.when(me > 0)
            def _():
                complete(turn_at)

            @pl.when(me == 0)
            def _():
                for g in range(QUERY_PER_KEY):
                    settle(turn_at, g, held[g][turn_at])

        pass_on(turn_at, 2)
        return carry

    lax.fori_loop(0, SETTLED + kheads, rounds, 0)

    def finish(h, carry):
        for index, ((slot, step), senders) in enumerate(plan):
            @pl.when(sends(senders, h))
            def _():
                copy_of(index, slot, step, h).wait_send()

        return carry

    lax.fori_loop(0, kheads, finish, 0)


def local(blocks, lanes, queries, keys, values, positions, doc_lengths):
    rows = queries.shape[0]
    kheads = keys.shape[1] // HEAD_SIZE
    count = blocks * lanes
    window = count // 2
    plan = routes(blocks, lanes)
    vmem = pl.BlockSpec(memory_space=pltpu.VMEM)
    anywhere = pl.BlockSpec(memory_space=pl.ANY)
    freq = jnp.asarray(frequencies())
    return pl.pallas_call(
        functools.partial(kernel, plan, lanes, count, window, kheads),
        out_shape=pltpu.VMEM(queries.shape, jnp.bfloat16),
        in_specs=[pl.BlockSpec(memory_space=pltpu.SMEM)] + [anywhere] * 5,
        out_specs=vmem,
        scratch_shapes=[
            pltpu.VMEM(positions.shape, jnp.int32),
            pltpu.VMEM(freq.shape, jnp.float32),
            pltpu.VMEM(keys.shape, jnp.bfloat16),
            pltpu.VMEM(values.shape, jnp.bfloat16),
            pltpu.VMEM((rows, HEAD_SIZE), jnp.float32),
            pltpu.VMEM((rows, HEAD_SIZE), jnp.float32),
            pltpu.VMEM((HEAD_SIZE // 2, rows), jnp.float32),
            pltpu.VMEM((HEAD_SIZE // 2, rows), jnp.float32),
            pltpu.VMEM((window + 1, kheads, 2 * rows, HEAD_SIZE), jnp.bfloat16),
            pltpu.VMEM((window + 1, rows, HEAD_SIZE), jnp.bfloat16),
            pltpu.VMEM((HEAD_SIZE, rows), jnp.bfloat16),
            pltpu.VMEM((rows, rows), jnp.bfloat16),
            pltpu.VMEM(queries.shape, jnp.bfloat16),
            pltpu.VMEM((kheads * QUERY_PER_KEY, HEAD_SIZE, rows), jnp.bfloat16),
            pltpu.VMEM((2, window - 1, rows, rows), jnp.float32),
            *[pltpu.VMEM((kheads, SUBLANES, rows), jnp.float32)] * QUERY_PER_KEY,
            *[pltpu.VMEM((kheads, HEAD_SIZE + SUBLANES, rows), jnp.float32)] * QUERY_PER_KEY,
            pltpu.SemaphoreType.DMA,
            pltpu.SemaphoreType.DMA((4,)),
            pltpu.SemaphoreType.DMA((len(plan), kheads)),
            pltpu.SemaphoreType.DMA((window + 1, kheads)),
        ],
        compiler_params=pltpu.CompilerParams(
            collective_id=0, has_side_effects=True, vmem_limit_bytes=60 * 1024 * 1024
        ),
        name="windowed_attention",
    )(doc_lengths, positions, freq, keys, values, queries)


def solution(mesh):
    in_specs = (
        P(("seq", "blk", "uly"), None),
        P(("seq", "blk", "uly"), None),
        P(("seq", "blk", "uly"), None),
        P(None, ("seq", "blk", "uly")),
        P("seq"),
    )
    out_specs = P(("seq", "blk", "uly"), None)
    body = functools.partial(local, mesh.shape["blk"], mesh.shape["uly"])
    return jax.shard_map(body, mesh=mesh, in_specs=in_specs, out_specs=out_specs, check_vma=False)
```

```python
import functools
import math

import jax
import jax.numpy as jnp
import numpy as np
from jax import lax
from jax.experimental import pallas as pl
from jax.experimental.pallas import tpu as pltpu
from jax.sharding import PartitionSpec as P

HEAD_SIZE = 128
QUERY_PER_KEY = 5
BURST = 8
SETTLED = 5
FAR = -1e30
SUBLANES = 8
SCORES_FIRST = 5


TABLE = {
    "own": {
        1: (
            (8, 4, 2, 0, 8, 8, 2, 0),
            (8, 4, 2, 0, 8, 8, 2, 0),
            (8, 4, 2, 0, 8, 8, 2, 0),
        ),
        2: (
            (5, 8, 0, 0, 5, 5, 0, 0),
            (5, 8, 0, 0, 5, 5, 0, 0),
            (5, 8, 0, 0, 5, 5, 0, 0),
        ),
        4: (
            (8, 8, 6, 3, 0, 0, 0, 0),
            (8, 8, 6, 3, 0, 0, 0, 0),
            (8, 8, 6, 3, 0, 0, 0, 0),
        ),
    },
    "relay": {
        4: (
            ((0, 0, 0, 0, 0, 6, 2, 2), (0, 0, 0, 0, 0, 1, 0, 0)),
            ((0, 0, 0, 0, 0, 6, 2, 2), (0, 0, 0, 0, 0, 1, 0, 0)),
        ),
        3: (
            ((0, 0, 0, 0, 0, 0, 1, 0), (0, 0, 0, 0, 0, 0, 2, 0)),
            ((0, 0, 0, 0, 0, 0, 1, 0), (0, 0, 0, 0, 0, 0, 2, 0)),
        ),
        1: (
            ((0, 0, 0, 0, 0, 2, 0, 0), (0, 1, 0, 1, 0, 1, 0, 0)),
            ((0, 0, 0, 0, 0, 2, 0, 0), (0, 1, 0, 1, 0, 1, 0, 0)),
        ),
    },
    "first": (1, 2, 3, 3, 3, 4, 2, 2),
}


def frequencies():
    pair = np.arange(HEAD_SIZE // 2)
    value = np.power(1000000.0, -2.0 * pair / HEAD_SIZE).astype(np.float32)
    return np.repeat(value[:, None], HEAD_SIZE, axis=1)


def rotary_tables(places, freq):
    rows = places.shape[1]
    half = HEAD_SIZE // 2
    pair = lax.broadcasted_iota(jnp.int32, (half, rows), 0)
    first = HEAD_SIZE // 8
    second = first + 3 * HEAD_SIZE // 16
    place = places.astype(jnp.float32)
    chosen = jnp.where(pair < first, place[0:1], jnp.where(pair < second, place[1:2], place[2:3]))
    angle = chosen * jnp.concatenate([freq] * (rows // HEAD_SIZE), axis=1)
    turns = jnp.floor(angle * (2.0 / math.pi) + 0.5)
    rest = angle - turns * 1.5703125
    rest = rest - turns * 4.8351287841796875e-4
    rest = rest - turns * 3.138552419841289520264e-7
    rest = rest - turns * 6.07710050630396597660e-11
    quarter = turns.astype(jnp.int32) & 3
    square = rest * rest
    sine = rest + rest * square * (
        -1.0 / 6 + square * (1.0 / 120 + square * (-1.0 / 5040 + square * (1.0 / 362880)))
    )
    cosine = 1.0 + square * (
        -0.5 + square * (1.0 / 24 + square * (-1.0 / 720 + square * (1.0 / 40320)))
    )
    swap = (quarter & 1) == 1
    sin_turned = jnp.where(swap, cosine, sine)
    cos_turned = jnp.where(swap, sine, cosine)
    sin_turned = jnp.where(quarter >= 2, -sin_turned, sin_turned)
    cos_turned = jnp.where((quarter == 1) | (quarter == 2), -cos_turned, cos_turned)
    return cos_turned, sin_turned


def routes(blocks, lanes):
    count = blocks * lanes
    window = count // 2

    def place(r):
        return (r // lanes // 2, r % lanes), r // lanes % 2

    def member(chip, core):
        return (chip[0] * 2 + core) * lanes + chip[1]

    found = {}
    for s in range(count):
        home, own_core = place(s)
        wanting = set(range(s + 1, min(count, s + window + 1)))

        def entry(chip):
            if chip == home:
                return s
            for core in (own_core, 1 - own_core):
                if member(chip, core) in wanting:
                    return member(chip, core)
            return None

        for half in (0, 1):
            for r in sorted(wanting):
                chip, _ = place(r)
                source = entry(chip)
                if source == r:
                    options = []
                    if chip[1] != home[1]:
                        options.append(entry((chip[0], home[1])))
                    if chip[0] > home[0]:
                        options.append(entry((chip[0] - 1, chip[1])))
                    if half:
                        options.reverse()
                    options = [o for o in options if o is not None] + [s]
                    source = options[0]
                found.setdefault((source - s, r - source), (set(), set()))[half].add(source)
    return sorted(found.items(), key=lambda item: (-item[0][0], item[0][1]))


def pick(me, values):
    found = jnp.int32(values[0])
    for device, value in enumerate(values):
        if value != values[0]:
            found = jnp.where(me == device, jnp.int32(value), found)
    return found


def timetable(blocks, lanes, window):
    if (blocks, lanes) == (4, 2):
        return TABLE
    return {
        "own": {step: ((3,),) * 3 for step in range(1, blocks * lanes)},
        "relay": {slot: (((0,), (0,)),) * 2 for slot in range(1, window + 1)},
        "first": (0,),
    }


def among(me, devices):
    hit = jnp.bool_(False)
    for device in sorted(devices):
        hit = hit | (me == device)
    return hit


def kernel(
    plan, lanes, count, window, kheads,
    lengths, places_in, freq_in, keys_in, values_in, queries, out,
    places, freq, keys, values, cosine, sine, cosine_t, sine_t, kv, kfeat, qfeat, tri, qbuf, qt, scores, *rest,
):
    best, held = rest[:QUERY_PER_KEY], rest[QUERY_PER_KEY : 2 * QUERY_PER_KEY]
    q_sem, in_sem, send_sem, recv_sem = rest[2 * QUERY_PER_KEY :]
    rows = keys.shape[0]
    size = HEAD_SIZE
    group = QUERY_PER_KEY * size
    me = lax.axis_index("blk") * lanes + lax.axis_index("uly")

    def where_is(r):
        return {"blk": lax.div(r, lanes), "uly": lax.rem(r, lanes)}

    barrier = pltpu.get_barrier_semaphore()
    for offset in range(1, count):
        peer = lax.rem(me + offset, count)
        pl.semaphore_signal(
            barrier, inc=1, device_id=where_is(peer), device_id_type=pl.DeviceIdType.MESH
        )
    loads = [
        pltpu.make_async_copy(source, target, in_sem.at[i])
        for i, (source, target) in enumerate(
            ((places_in, places), (freq_in, freq), (keys_in, keys), (values_in, values))
        )
    ]
    for load in loads:
        load.start()
    fetch = pltpu.make_async_copy(queries, qbuf, q_sem)
    fetch.start()

    def column(h, width):
        return pl.ds(pl.multiple_of(h * width, width), width)

    loads[0].wait()
    loads[1].wait()
    cos_half, sin_half = rotary_tables(places[...], freq[...])
    cosine_t[...] = cos_half
    sine_t[...] = sin_half
    cosine[...] = jnp.concatenate([cos_half, cos_half], axis=0).T
    sine[...] = jnp.concatenate([-sin_half, sin_half], axis=0).T

    def turn(x):
        x = x.astype(jnp.float32)
        return (x * cosine[...] + pltpu.roll(x, size // 2, 1) * sine[...]).astype(jnp.bfloat16)

    loads[2].wait()
    loads[3].wait()

    def own_block(h, carry):
        kv[0, h, :rows, :] = turn(keys[:, column(h, size)])
        turned = values[:, column(h, size)].astype(jnp.float32).T.astype(jnp.bfloat16)
        for piece in range(rows // size):
            at = rows + piece * size
            kv[0, h, at : at + size, :] = turned[:, piece * size : (piece + 1) * size]
        return carry

    lax.fori_loop(0, kheads, own_block, 0)
    pl.semaphore_wait(barrier, count - 1)

    def copy_of(index, slot, step, h):
        return pltpu.make_async_remote_copy(
            src_ref=kv.at[slot, h],
            dst_ref=kv.at[slot + step, h],
            send_sem=send_sem.at[index, h],
            recv_sem=recv_sem.at[slot + step, h],
            device_id=where_is(me + step),
            device_id_type=pl.DeviceIdType.MESH,
        )

    def arrival(slot, h):
        return pltpu.make_async_remote_copy(
            src_ref=kv.at[slot, h],
            dst_ref=kv.at[slot, h],
            send_sem=send_sem.at[0, h],
            recv_sem=recv_sem.at[slot, h],
            device_id=where_is(me),
            device_id_type=pl.DeviceIdType.MESH,
        )

    table = timetable(count // lanes, lanes, window)
    half = kheads // 2
    quarters = (0, half, kheads * 3 // 4, kheads)

    def span(senders):
        low, high = (among(me, devices) for devices in senders)
        return jnp.where(low, 0, half), jnp.where(high, kheads, half)

    spans = [span(senders) for _, senders in plan]
    relayed = {}
    for slot in range(1, window + 1):
        ours = [senders for (from_slot, _), senders in plan if from_slot == slot]
        relayed[slot] = span([set().union(*(s[part] for s in ours)) for part in (0, 1)])

    def relays(slot, h):
        return (h >= relayed[slot][0]) & (h < relayed[slot][1])

    own_turns = []
    for index, ((slot, step), _) in enumerate(plan):
        leads = table["own"][step] if slot == 0 else ()
        edges = quarters
        if len(set(leads)) == 1:
            leads, edges = leads[:1], (0, kheads)
        for part, lead in enumerate(leads):
            ahead = pick(me, lead)
            start = jnp.maximum(spans[index][0], edges[part]) - ahead
            stop = jnp.minimum(spans[index][1], edges[part + 1]) - ahead
            own_turns.append((index, step, ahead, start, stop))

    relay_turns = []
    for slot in sorted({slot for (slot, _), _ in plan if slot}, reverse=True):
        turns, edges = table["relay"][slot], (0, half, kheads)
        if len(set(turns)) == 1:
            turns, edges = turns[:1], (0, kheads)
        for part, (lead, at) in enumerate(turns):
            ahead, where = pick(me, lead), pick(me, at)
            start = jnp.maximum(relayed[slot][0], edges[part]) - ahead
            stop = jnp.minimum(relayed[slot][1], edges[part + 1]) - ahead
            for place in sorted(set(at)):
                stop_here = jnp.where(where == place, stop, start)
                relay_turns.append((place, slot, ahead, start, stop_here))

    def due(turn_at, turns):
        hit = jnp.bool_(False)
        for *_, start, stop in turns:
            hit = hit | ((turn_at >= start) & (turn_at < stop))
        return hit

    def send_own(turn_at):
        @pl.when(due(turn_at, own_turns))
        def _():
            for index, step, ahead, start, stop in own_turns:
                @pl.when((turn_at >= start) & (turn_at < stop))
                def _():
                    copy_of(index, 0, step, turn_at + ahead).start()

    def pass_on(turn_at, place):
        turns = [turn[1:] for turn in relay_turns if turn[0] == place]

        @pl.when(due(turn_at, turns))
        def _():
            for slot, ahead, start, stop in turns:
                @pl.when((turn_at >= start) & (turn_at < stop))
                def _():
                    h = turn_at + ahead
                    arrival(slot, h).wait_recv()
                    for index, ((from_slot, step), _) in enumerate(plan):
                        if from_slot == slot:
                            @pl.when((h >= spans[index][0]) & (h < spans[index][1]))
                            def _():
                                copy_of(index, slot, step, h).start()

    def opening(i, carry):
        turn_at = i - BURST
        send_own(turn_at)
        for place in range(3):
            pass_on(turn_at, place)
        return carry

    lax.fori_loop(0, BURST - SETTLED, opening, 0)

    for slot in range(1, window + 1):
        @pl.when(me < slot)
        def _():
            def clear(h, carry):
                kv[slot, h] = jnp.zeros((rows + rows // size * size, size), kv.dtype)
                return carry

            lax.fori_loop(0, kheads, clear, 0)

    lane = lax.broadcasted_iota(jnp.int32, (1, size), 1)
    opens = jnp.zeros((1, size), jnp.int32)
    closes = jnp.zeros((1, size), jnp.int32)
    end = jnp.int32(0)
    for d in range(lengths.shape[0]):
        start, end = end, end + lengths[d]
        opens = jnp.where(lane == d, start, opens)
        closes = jnp.where(lane == d, end, closes)
    row = lax.broadcasted_iota(jnp.int32, (rows, size), 0)
    for slot in range(window + 1):
        token = row + (me - slot) * rows
        inside = (token >= opens) & (token < closes)
        kfeat[slot] = jnp.where(inside, 0.0, FAR).astype(jnp.bfloat16)
        if slot == 0:
            qfeat[...] = jnp.where(inside, 1.0, 0.0).T.astype(jnp.bfloat16)
    key_at = lax.broadcasted_iota(jnp.int32, (rows, rows), 0)
    query_at = lax.broadcasted_iota(jnp.int32, (rows, rows), 1)
    tri[...] = jnp.where(key_at <= query_at, 1.0, 0.0).astype(jnp.bfloat16)

    fetch.wait()

    def turn_queries(h, carry):
        x = qbuf[:, column(h, size)].astype(jnp.float32).T
        low, high = x[: size // 2], x[size // 2 :]
        cos_half, sin_half = cosine_t[...], sine_t[...]
        turned = jnp.concatenate(
            [low * cos_half - high * sin_half, high * cos_half + low * sin_half], axis=0
        )
        qt[h] = turned.astype(jnp.bfloat16)
        return carry

    lax.fori_loop(0, kheads * QUERY_PER_KEY, turn_queries, 0, unroll=QUERY_PER_KEY)

    scale = math.log2(math.e) / math.sqrt(size)
    ones = jnp.ones((2 * SUBLANES, rows), jnp.bfloat16)

    def key_of(slot, h):
        return jnp.concatenate([kv[slot, h, :rows, :], kfeat[slot]], axis=1)

    def value_of(slot, h):
        pieces = [
            kv[slot, h, rows + p * size : rows + (p + 1) * size, :] for p in range(rows // size)
        ]
        return jnp.concatenate([jnp.concatenate(pieces, axis=1), ones], axis=0)

    def query_of(h, g):
        return jnp.concatenate([qt[h * QUERY_PER_KEY + g], qfeat[...]], axis=0)

    def dot(a, b):
        return jnp.dot(a, b, preferred_element_type=jnp.float32)

    def begin(h):
        scores = []
        for g in range(QUERY_PER_KEY):
            q = query_of(h, g)
            scores.append(
                jnp.where(key_at <= query_at, dot(key_of(0, h), q), dot(key_of(window, h), q))
            )
        pending = None
        for g in range(QUERY_PER_KEY + 1):
            if g < QUERY_PER_KEY:
                top = jnp.max(scores[g], axis=0, keepdims=True)
                w = jnp.exp2((scores[g] - top) * scale).astype(jnp.bfloat16)
                near = w * tri[...]
                best[g][h] = jnp.broadcast_to(top, (SUBLANES, rows))
                both = dot(value_of(0, h), near) + dot(value_of(window, h), w - near)
            if pending is not None:
                held[g - 1][h] = pending[: size + SUBLANES]
            pending = both

    def complete(h):
        def score(g):
            q = query_of(h, g)
            top = best[g][h][:1]
            for slot in range(1, window):
                s = dot(key_of(slot, h), q)
                scores[g, slot - 1] = s
                top = jnp.maximum(top, jnp.max(s, axis=0, keepdims=True))
            return top

        def attend(g, top):
            keep = jnp.exp2((best[g][h][:1] - top) * scale)
            both = None
            for slot in range(1, window):
                w = jnp.exp2((scores[g, slot - 1] - top) * scale).astype(jnp.bfloat16)
                part = dot(value_of(slot, h), w)
                both = part if both is None else both + part
            return both[: size + SUBLANES] + held[g][h] * keep

        tops = [score(g) for g in range(SCORES_FIRST)]
        pending = None
        for g in range(QUERY_PER_KEY):
            if g + SCORES_FIRST < QUERY_PER_KEY:
                tops.append(score(g + SCORES_FIRST))
            both = attend(g, tops[g])
            if pending is not None:
                settle(h, g - 1, pending)
            pending = both
        settle(h, QUERY_PER_KEY - 1, pending)

    def settle(h, g, both):
        result = both[:size] * (1.0 / both[size : size + 1])
        at = pl.ds(pl.multiple_of(h * group + g * size, size), size)
        out[:, at] = result.T.astype(jnp.bfloat16)

    def take(slot, h):
        @pl.when((me >= slot) & jnp.logical_not(relays(slot, h)))
        def _():
            arrival(slot, h).wait_recv()

    def rounds(i, carry):
        turn_at = i - SETTLED
        send_own(turn_at)
        pass_on(turn_at, 0)
        first = turn_at + pick(me, table["first"])

        @pl.when((first >= 0) & (first < kheads))
        def _():
            take(window, first)
            begin(first)

        pass_on(turn_at, 1)

        @pl.when(turn_at >= 0)
        def _():
            for slot in range(1, window):
                take(slot, turn_at)

            complete(turn_at)

        pass_on(turn_at, 2)
        return carry

    lax.fori_loop(0, SETTLED + kheads, rounds, 0)

    def finish(h, carry):
        for index, ((slot, step), senders) in enumerate(plan):
            @pl.when((h >= spans[index][0]) & (h < spans[index][1]))
            def _():
                copy_of(index, slot, step, h).wait_send()

        return carry

    lax.fori_loop(0, kheads, finish, 0)


def local(blocks, lanes, queries, keys, values, positions, doc_lengths):
    rows = queries.shape[0]
    kheads = keys.shape[1] // HEAD_SIZE
    count = blocks * lanes
    window = count // 2
    plan = routes(blocks, lanes)
    vmem = pl.BlockSpec(memory_space=pltpu.VMEM)
    anywhere = pl.BlockSpec(memory_space=pl.ANY)
    freq = jnp.asarray(frequencies())
    return pl.pallas_call(
        functools.partial(kernel, plan, lanes, count, window, kheads),
        out_shape=pltpu.VMEM(queries.shape, jnp.bfloat16),
        in_specs=[pl.BlockSpec(memory_space=pltpu.SMEM)] + [anywhere] * 5,
        out_specs=vmem,
        scratch_shapes=[
            pltpu.VMEM(positions.shape, jnp.int32),
            pltpu.VMEM(freq.shape, jnp.float32),
            pltpu.VMEM(keys.shape, jnp.bfloat16),
            pltpu.VMEM(values.shape, jnp.bfloat16),
            pltpu.VMEM((rows, HEAD_SIZE), jnp.float32),
            pltpu.VMEM((rows, HEAD_SIZE), jnp.float32),
            pltpu.VMEM((HEAD_SIZE // 2, rows), jnp.float32),
            pltpu.VMEM((HEAD_SIZE // 2, rows), jnp.float32),
            pltpu.VMEM((window + 1, kheads, 2 * rows, HEAD_SIZE), jnp.bfloat16),
            pltpu.VMEM((window + 1, rows, HEAD_SIZE), jnp.bfloat16),
            pltpu.VMEM((HEAD_SIZE, rows), jnp.bfloat16),
            pltpu.VMEM((rows, rows), jnp.bfloat16),
            pltpu.VMEM(queries.shape, jnp.bfloat16),
            pltpu.VMEM((kheads * QUERY_PER_KEY, HEAD_SIZE, rows), jnp.bfloat16),
            pltpu.VMEM((QUERY_PER_KEY, window - 1, rows, rows), jnp.float32),
            *[pltpu.VMEM((kheads, SUBLANES, rows), jnp.float32)] * QUERY_PER_KEY,
            *[pltpu.VMEM((kheads, HEAD_SIZE + SUBLANES, rows), jnp.float32)] * QUERY_PER_KEY,
            pltpu.SemaphoreType.DMA,
            pltpu.SemaphoreType.DMA((4,)),
            pltpu.SemaphoreType.DMA((len(plan), kheads)),
            pltpu.SemaphoreType.DMA((window + 1, kheads)),
        ],
        compiler_params=pltpu.CompilerParams(
            collective_id=0, has_side_effects=True, vmem_limit_bytes=60 * 1024 * 1024
        ),
        name="windowed_attention",
    )(doc_lengths, positions, freq, keys, values, queries)


def solution(mesh):
    in_specs = (
        P(("seq", "blk", "uly"), None),
        P(("seq", "blk", "uly"), None),
        P(("seq", "blk", "uly"), None),
        P(None, ("seq", "blk", "uly")),
        P("seq"),
    )
    out_specs = P(("seq", "blk", "uly"), None)
    body = functools.partial(local, mesh.shape["blk"], mesh.shape["uly"])
    return jax.shard_map(body, mesh=mesh, in_specs=in_specs, out_specs=out_specs, check_vma=False)
```

```python
import functools
import math

import jax
import jax.numpy as jnp
import numpy as np
from jax import lax
from jax.experimental import pallas as pl
from jax.experimental.pallas import tpu as pltpu
from jax.sharding import PartitionSpec as P

HEAD_SIZE = 128
QUERY_PER_KEY = 5
BURST = 8
SETTLED = 5
FAR = -1e30
SUBLANES = 8
SCORES_FIRST = 5


TABLE = {
    "own": {
        1: (
            (8, 4, 2, 0, 8, 8, 2, 0),
            (8, 4, 2, 0, 8, 8, 2, 0),
            (8, 4, 2, 0, 8, 8, 2, 0),
        ),
        2: (
            (5, 8, 0, 0, 5, 5, 0, 0),
            (5, 8, 0, 0, 5, 5, 0, 0),
            (5, 8, 0, 0, 5, 5, 0, 0),
        ),
        4: (
            (8, 8, 6, 2, 0, 0, 0, 0),
            (8, 8, 6, 2, 0, 0, 0, 0),
            (8, 8, 6, 2, 0, 0, 0, 0),
        ),
    },
    "relay": {
        4: (
            ((0, 0, 0, 0, 0, 6, 2, 2), (0, 0, 0, 0, 0, 1, 0, 0)),
            ((0, 0, 0, 0, 0, 6, 2, 2), (0, 0, 0, 0, 0, 1, 0, 0)),
        ),
        3: (
            ((0, 0, 0, 0, 0, 0, 1, 0), (0, 0, 0, 0, 0, 0, 2, 0)),
            ((0, 0, 0, 0, 0, 0, 1, 0), (0, 0, 0, 0, 0, 0, 2, 0)),
        ),
        1: (
            ((0, 0, 0, 0, 0, 2, 0, 0), (0, 1, 0, 1, 0, 1, 0, 0)),
            ((0, 0, 0, 0, 0, 2, 0, 0), (0, 1, 0, 1, 0, 1, 0, 0)),
        ),
    },
    "first": (1, 2, 3, 3, 3, 4, 2, 2),
}


def frequencies():
    pair = np.arange(HEAD_SIZE // 2)
    value = np.power(1000000.0, -2.0 * pair / HEAD_SIZE).astype(np.float32)
    return np.repeat(value[:, None], HEAD_SIZE, axis=1)


def rotary_tables(places, freq):
    rows = places.shape[1]
    half = HEAD_SIZE // 2
    pair = lax.broadcasted_iota(jnp.int32, (half, rows), 0)
    first = HEAD_SIZE // 8
    second = first + 3 * HEAD_SIZE // 16
    place = places.astype(jnp.float32)
    chosen = jnp.where(pair < first, place[0:1], jnp.where(pair < second, place[1:2], place[2:3]))
    angle = chosen * jnp.concatenate([freq] * (rows // HEAD_SIZE), axis=1)
    turns = jnp.floor(angle * (2.0 / math.pi) + 0.5)
    rest = angle - turns * 1.5703125
    rest = rest - turns * 4.8351287841796875e-4
    rest = rest - turns * 3.138552419841289520264e-7
    rest = rest - turns * 6.07710050630396597660e-11
    quarter = turns.astype(jnp.int32) & 3
    square = rest * rest
    sine = rest + rest * square * (
        -1.0 / 6 + square * (1.0 / 120 + square * (-1.0 / 5040 + square * (1.0 / 362880)))
    )
    cosine = 1.0 + square * (
        -0.5 + square * (1.0 / 24 + square * (-1.0 / 720 + square * (1.0 / 40320)))
    )
    swap = (quarter & 1) == 1
    sin_turned = jnp.where(swap, cosine, sine)
    cos_turned = jnp.where(swap, sine, cosine)
    sin_turned = jnp.where(quarter >= 2, -sin_turned, sin_turned)
    cos_turned = jnp.where((quarter == 1) | (quarter == 2), -cos_turned, cos_turned)
    return cos_turned, sin_turned


def routes(blocks, lanes):
    count = blocks * lanes
    window = count // 2

    def place(r):
        return (r // lanes // 2, r % lanes), r // lanes % 2

    def member(chip, core):
        return (chip[0] * 2 + core) * lanes + chip[1]

    found = {}
    for s in range(count):
        home, own_core = place(s)
        wanting = set(range(s + 1, min(count, s + window + 1)))

        def entry(chip):
            if chip == home:
                return s
            for core in (own_core, 1 - own_core):
                if member(chip, core) in wanting:
                    return member(chip, core)
            return None

        for half in (0, 1):
            for r in sorted(wanting):
                chip, _ = place(r)
                source = entry(chip)
                if source == r:
                    options = []
                    if chip[1] != home[1]:
                        options.append(entry((chip[0], home[1])))
                    if chip[0] > home[0]:
                        options.append(entry((chip[0] - 1, chip[1])))
                    if half:
                        options.reverse()
                    options = [o for o in options if o is not None] + [s]
                    source = options[0]
                found.setdefault((source - s, r - source), (set(), set()))[half].add(source)
    return sorted(found.items(), key=lambda item: (-item[0][0], item[0][1]))


def pick(me, values):
    found = jnp.int32(values[0])
    for device, value in enumerate(values):
        if value != values[0]:
            found = jnp.where(me == device, jnp.int32(value), found)
    return found


def timetable(blocks, lanes, window):
    if (blocks, lanes) == (4, 2):
        return TABLE
    return {
        "own": {step: ((3,),) * 3 for step in range(1, blocks * lanes)},
        "relay": {slot: (((0,), (0,)),) * 2 for slot in range(1, window + 1)},
        "first": (0,),
    }


def among(me, devices):
    hit = jnp.bool_(False)
    for device in sorted(devices):
        hit = hit | (me == device)
    return hit


def kernel(
    plan, lanes, count, window, kheads,
    lengths, places_in, freq_in, keys_in, values_in, queries, out,
    places, freq, keys, values, cosine, sine, cosine_t, sine_t, kv, kfeat, qfeat, tri, qbuf, qt, scores, *rest,
):
    best, held = rest[:QUERY_PER_KEY], rest[QUERY_PER_KEY : 2 * QUERY_PER_KEY]
    q_sem, in_sem, send_sem, recv_sem = rest[2 * QUERY_PER_KEY :]
    rows = keys.shape[0]
    size = HEAD_SIZE
    group = QUERY_PER_KEY * size
    me = lax.axis_index("blk") * lanes + lax.axis_index("uly")

    def where_is(r):
        return {"blk": lax.div(r, lanes), "uly": lax.rem(r, lanes)}

    barrier = pltpu.get_barrier_semaphore()
    for offset in range(1, count):
        peer = lax.rem(me + offset, count)
        pl.semaphore_signal(
            barrier, inc=1, device_id=where_is(peer), device_id_type=pl.DeviceIdType.MESH
        )
    loads = [
        pltpu.make_async_copy(source, target, in_sem.at[i])
        for i, (source, target) in enumerate(
            ((places_in, places), (freq_in, freq), (keys_in, keys), (values_in, values))
        )
    ]
    for load in loads:
        load.start()
    fetch = pltpu.make_async_copy(queries, qbuf, q_sem)
    fetch.start()

    def column(h, width):
        return pl.ds(pl.multiple_of(h * width, width), width)

    loads[0].wait()
    loads[1].wait()
    cos_half, sin_half = rotary_tables(places[...], freq[...])
    cosine_t[...] = cos_half
    sine_t[...] = sin_half
    cosine[...] = jnp.concatenate([cos_half, cos_half], axis=0).T
    sine[...] = jnp.concatenate([-sin_half, sin_half], axis=0).T

    def turn(x):
        x = x.astype(jnp.float32)
        return (x * cosine[...] + pltpu.roll(x, size // 2, 1) * sine[...]).astype(jnp.bfloat16)

    loads[2].wait()
    loads[3].wait()

    def own_block(h, carry):
        kv[0, h, :rows, :] = turn(keys[:, column(h, size)])
        turned = values[:, column(h, size)].astype(jnp.float32).T.astype(jnp.bfloat16)
        for piece in range(rows // size):
            at = rows + piece * size
            kv[0, h, at : at + size, :] = turned[:, piece * size : (piece + 1) * size]
        return carry

    lax.fori_loop(0, kheads, own_block, 0)
    pl.semaphore_wait(barrier, count - 1)

    def copy_of(index, slot, step, h):
        return pltpu.make_async_remote_copy(
            src_ref=kv.at[slot, h],
            dst_ref=kv.at[slot + step, h],
            send_sem=send_sem.at[index, h],
            recv_sem=recv_sem.at[slot + step, h],
            device_id=where_is(me + step),
            device_id_type=pl.DeviceIdType.MESH,
        )

    def arrival(slot, h):
        return pltpu.make_async_remote_copy(
            src_ref=kv.at[slot, h],
            dst_ref=kv.at[slot, h],
            send_sem=send_sem.at[0, h],
            recv_sem=recv_sem.at[slot, h],
            device_id=where_is(me),
            device_id_type=pl.DeviceIdType.MESH,
        )

    table = timetable(count // lanes, lanes, window)
    half = kheads // 2
    quarters = (0, half, kheads * 3 // 4, kheads)

    def span(senders):
        low, high = (among(me, devices) for devices in senders)
        return jnp.where(low, 0, half), jnp.where(high, kheads, half)

    spans = [span(senders) for _, senders in plan]
    relayed = {}
    for slot in range(1, window + 1):
        ours = [senders for (from_slot, _), senders in plan if from_slot == slot]
        relayed[slot] = span([set().union(*(s[part] for s in ours)) for part in (0, 1)])

    def relays(slot, h):
        return (h >= relayed[slot][0]) & (h < relayed[slot][1])

    own_turns = []
    for index, ((slot, step), _) in enumerate(plan):
        leads = table["own"][step] if slot == 0 else ()
        edges = quarters
        if len(set(leads)) == 1:
            leads, edges = leads[:1], (0, kheads)
        for part, lead in enumerate(leads):
            ahead = pick(me, lead)
            start = jnp.maximum(spans[index][0], edges[part]) - ahead
            stop = jnp.minimum(spans[index][1], edges[part + 1]) - ahead
            own_turns.append((index, step, ahead, start, stop))

    relay_turns = []
    for slot in sorted({slot for (slot, _), _ in plan if slot}, reverse=True):
        turns, edges = table["relay"][slot], (0, half, kheads)
        if len(set(turns)) == 1:
            turns, edges = turns[:1], (0, kheads)
        for part, (lead, at) in enumerate(turns):
            ahead, where = pick(me, lead), pick(me, at)
            start = jnp.maximum(relayed[slot][0], edges[part]) - ahead
            stop = jnp.minimum(relayed[slot][1], edges[part + 1]) - ahead
            for place in sorted(set(at)):
                stop_here = jnp.where(where == place, stop, start)
                relay_turns.append((place, slot, ahead, start, stop_here))

    def due(turn_at, turns):
        hit = jnp.bool_(False)
        for *_, start, stop in turns:
            hit = hit | ((turn_at >= start) & (turn_at < stop))
        return hit

    def send_own(turn_at):
        @pl.when(due(turn_at, own_turns))
        def _():
            for index, step, ahead, start, stop in own_turns:
                @pl.when((turn_at >= start) & (turn_at < stop))
                def _():
                    copy_of(index, 0, step, turn_at + ahead).start()

    def pass_on(turn_at, place):
        turns = [turn[1:] for turn in relay_turns if turn[0] == place]

        @pl.when(due(turn_at, turns))
        def _():
            for slot, ahead, start, stop in turns:
                @pl.when((turn_at >= start) & (turn_at < stop))
                def _():
                    h = turn_at + ahead
                    arrival(slot, h).wait_recv()
                    for index, ((from_slot, step), _) in enumerate(plan):
                        if from_slot == slot:
                            @pl.when((h >= spans[index][0]) & (h < spans[index][1]))
                            def _():
                                copy_of(index, slot, step, h).start()

    def opening(i, carry):
        turn_at = i - BURST
        send_own(turn_at)
        for place in range(3):
            pass_on(turn_at, place)
        return carry

    lax.fori_loop(0, BURST - SETTLED, opening, 0)

    for slot in range(1, window + 1):
        @pl.when(me < slot)
        def _():
            def clear(h, carry):
                kv[slot, h] = jnp.zeros((rows + rows // size * size, size), kv.dtype)
                return carry

            lax.fori_loop(0, kheads, clear, 0)

    lane = lax.broadcasted_iota(jnp.int32, (1, size), 1)
    opens = jnp.zeros((1, size), jnp.int32)
    closes = jnp.zeros((1, size), jnp.int32)
    end = jnp.int32(0)
    for d in range(lengths.shape[0]):
        start, end = end, end + lengths[d]
        opens = jnp.where(lane == d, start, opens)
        closes = jnp.where(lane == d, end, closes)
    row = lax.broadcasted_iota(jnp.int32, (rows, size), 0)
    for slot in range(window + 1):
        token = row + (me - slot) * rows
        inside = (token >= opens) & (token < closes)
        kfeat[slot] = jnp.where(inside, 0.0, FAR).astype(jnp.bfloat16)
        if slot == 0:
            qfeat[...] = jnp.where(inside, 1.0, 0.0).T.astype(jnp.bfloat16)
    key_at = lax.broadcasted_iota(jnp.int32, (rows, rows), 0)
    query_at = lax.broadcasted_iota(jnp.int32, (rows, rows), 1)
    tri[...] = jnp.where(key_at <= query_at, 1.0, 0.0).astype(jnp.bfloat16)

    fetch.wait()

    def turn_queries(h, carry):
        x = qbuf[:, column(h, size)].astype(jnp.float32).T
        low, high = x[: size // 2], x[size // 2 :]
        cos_half, sin_half = cosine_t[...], sine_t[...]
        turned = jnp.concatenate(
            [low * cos_half - high * sin_half, high * cos_half + low * sin_half], axis=0
        )
        qt[h] = turned.astype(jnp.bfloat16)
        return carry

    lax.fori_loop(0, kheads * QUERY_PER_KEY, turn_queries, 0, unroll=QUERY_PER_KEY)

    scale = math.log2(math.e) / math.sqrt(size)
    ones = jnp.ones((2 * SUBLANES, rows), jnp.bfloat16)

    def key_of(slot, h):
        return jnp.concatenate([kv[slot, h, :rows, :], kfeat[slot]], axis=1)

    def value_of(slot, h):
        pieces = [
            kv[slot, h, rows + p * size : rows + (p + 1) * size, :] for p in range(rows // size)
        ]
        return jnp.concatenate([jnp.concatenate(pieces, axis=1), ones], axis=0)

    def query_of(h, g):
        return jnp.concatenate([qt[h * QUERY_PER_KEY + g], qfeat[...]], axis=0)

    def dot(a, b):
        return jnp.dot(a, b, preferred_element_type=jnp.float32)

    def begin(h):
        scores = []
        for g in range(QUERY_PER_KEY):
            q = query_of(h, g)
            scores.append(
                jnp.where(key_at <= query_at, dot(key_of(0, h), q), dot(key_of(window, h), q))
            )
        pending = None
        for g in range(QUERY_PER_KEY + 1):
            if g < QUERY_PER_KEY:
                top = jnp.max(scores[g], axis=0, keepdims=True)
                w = jnp.exp2((scores[g] - top) * scale).astype(jnp.bfloat16)
                near = w * tri[...]
                best[g][h] = jnp.broadcast_to(top, (SUBLANES, rows))
                both = dot(value_of(0, h), near) + dot(value_of(window, h), w - near)
            if pending is not None:
                held[g - 1][h] = pending[: size + SUBLANES]
            pending = both

    def complete(h):
        def score(g):
            q = query_of(h, g)
            top = best[g][h][:1]
            for slot in range(1, window):
                s = dot(key_of(slot, h), q)
                scores[g, slot - 1] = s
                top = jnp.maximum(top, jnp.max(s, axis=0, keepdims=True))
            return top

        def attend(g, top):
            keep = jnp.exp2((best[g][h][:1] - top) * scale)
            both = None
            for slot in range(1, window):
                w = jnp.exp2((scores[g, slot - 1] - top) * scale).astype(jnp.bfloat16)
                part = dot(value_of(slot, h), w)
                both = part if both is None else both + part
            return both[: size + SUBLANES] + held[g][h] * keep

        tops = [score(g) for g in range(SCORES_FIRST)]
        pending = None
        for g in range(QUERY_PER_KEY):
            if g + SCORES_FIRST < QUERY_PER_KEY:
                tops.append(score(g + SCORES_FIRST))
            both = attend(g, tops[g])
            if pending is not None:
                settle(h, g - 1, pending)
            pending = both
        settle(h, QUERY_PER_KEY - 1, pending)

    def settle(h, g, both):
        result = both[:size] * (1.0 / both[size : size + 1])
        at = pl.ds(pl.multiple_of(h * group + g * size, size), size)
        out[:, at] = result.T.astype(jnp.bfloat16)

    def take(slot, h):
        @pl.when((me >= slot) & jnp.logical_not(relays(slot, h)))
        def _():
            arrival(slot, h).wait_recv()

    def rounds(i, carry):
        turn_at = i - SETTLED
        send_own(turn_at)
        pass_on(turn_at, 0)
        first = turn_at + pick(me, table["first"])

        @pl.when((first >= 0) & (first < kheads))
        def _():
            take(window, first)
            begin(first)

        pass_on(turn_at, 1)

        @pl.when(turn_at >= 0)
        def _():
            for slot in range(1, window):
                take(slot, turn_at)

            complete(turn_at)

        pass_on(turn_at, 2)
        return carry

    lax.fori_loop(0, SETTLED + kheads, rounds, 0)

    for index, ((slot, step), _) in enumerate(plan):
        def finish(h, carry):
            copy_of(index, slot, step, h).wait_send()
            return carry

        lax.fori_loop(spans[index][0], spans[index][1], finish, 0)


def local(blocks, lanes, queries, keys, values, positions, doc_lengths):
    rows = queries.shape[0]
    kheads = keys.shape[1] // HEAD_SIZE
    count = blocks * lanes
    window = count // 2
    plan = routes(blocks, lanes)
    vmem = pl.BlockSpec(memory_space=pltpu.VMEM)
    anywhere = pl.BlockSpec(memory_space=pl.ANY)
    freq = jnp.asarray(frequencies())
    return pl.pallas_call(
        functools.partial(kernel, plan, lanes, count, window, kheads),
        out_shape=pltpu.VMEM(queries.shape, jnp.bfloat16),
        in_specs=[pl.BlockSpec(memory_space=pltpu.SMEM)] + [anywhere] * 5,
        out_specs=vmem,
        scratch_shapes=[
            pltpu.VMEM(positions.shape, jnp.int32),
            pltpu.VMEM(freq.shape, jnp.float32),
            pltpu.VMEM(keys.shape, jnp.bfloat16),
            pltpu.VMEM(values.shape, jnp.bfloat16),
            pltpu.VMEM((rows, HEAD_SIZE), jnp.float32),
            pltpu.VMEM((rows, HEAD_SIZE), jnp.float32),
            pltpu.VMEM((HEAD_SIZE // 2, rows), jnp.float32),
            pltpu.VMEM((HEAD_SIZE // 2, rows), jnp.float32),
            pltpu.VMEM((window + 1, kheads, 2 * rows, HEAD_SIZE), jnp.bfloat16),
            pltpu.VMEM((window + 1, rows, HEAD_SIZE), jnp.bfloat16),
            pltpu.VMEM((HEAD_SIZE, rows), jnp.bfloat16),
            pltpu.VMEM((rows, rows), jnp.bfloat16),
            pltpu.VMEM(queries.shape, jnp.bfloat16),
            pltpu.VMEM((kheads * QUERY_PER_KEY, HEAD_SIZE, rows), jnp.bfloat16),
            pltpu.VMEM((QUERY_PER_KEY, window - 1, rows, rows), jnp.float32),
            *[pltpu.VMEM((kheads, SUBLANES, rows), jnp.float32)] * QUERY_PER_KEY,
            *[pltpu.VMEM((kheads, HEAD_SIZE + SUBLANES, rows), jnp.float32)] * QUERY_PER_KEY,
            pltpu.SemaphoreType.DMA,
            pltpu.SemaphoreType.DMA((4,)),
            pltpu.SemaphoreType.DMA((len(plan), kheads)),
            pltpu.SemaphoreType.DMA((window + 1, kheads)),
        ],
        compiler_params=pltpu.CompilerParams(
            collective_id=0, has_side_effects=True, vmem_limit_bytes=60 * 1024 * 1024
        ),
        name="windowed_attention",
    )(doc_lengths, positions, freq, keys, values, queries)


def solution(mesh):
    in_specs = (
        P(("seq", "blk", "uly"), None),
        P(("seq", "blk", "uly"), None),
        P(("seq", "blk", "uly"), None),
        P(None, ("seq", "blk", "uly")),
        P("seq"),
    )
    out_specs = P(("seq", "blk", "uly"), None)
    body = functools.partial(local, mesh.shape["blk"], mesh.shape["uly"])
    return jax.shard_map(body, mesh=mesh, in_specs=in_specs, out_specs=out_specs, check_vma=False)
```

```python
import functools
import math

import jax
import jax.numpy as jnp
import numpy as np
from jax import lax
from jax.experimental import pallas as pl
from jax.experimental.pallas import tpu as pltpu
from jax.sharding import PartitionSpec as P

HEAD_SIZE = 128
QUERY_PER_KEY = 5
BURST = 8
SETTLED = 5
FAR = -1e30
SUBLANES = 8
SCORES_FIRST = 5


TABLE = {
    "own": {
        1: (
            (8, 4, 2, 0, 8, 8, 2, 0),
            (8, 4, 2, 0, 8, 8, 2, 0),
            (8, 4, 2, 0, 8, 8, 2, 0),
        ),
        2: (
            (5, 8, 0, 0, 5, 5, 0, 0),
            (5, 8, 0, 0, 5, 5, 0, 0),
            (5, 8, 0, 0, 5, 5, 0, 0),
        ),
        4: (
            (8, 8, 6, 2, 0, 0, 0, 0),
            (8, 8, 6, 2, 0, 0, 0, 0),
            (8, 8, 6, 2, 0, 0, 0, 0),
        ),
    },
    "relay": {
        4: (
            ((0, 0, 0, 0, 0, 6, 2, 2), (0, 0, 0, 0, 0, 1, 0, 0)),
            ((0, 0, 0, 0, 0, 6, 2, 2), (0, 0, 0, 0, 0, 1, 0, 0)),
        ),
        3: (
            ((0, 0, 0, 0, 0, 0, 1, 0), (0, 0, 0, 0, 0, 0, 2, 0)),
            ((0, 0, 0, 0, 0, 0, 1, 0), (0, 0, 0, 0, 0, 0, 2, 0)),
        ),
        1: (
            ((0, 0, 0, 0, 0, 2, 0, 0), (0, 1, 0, 1, 0, 1, 0, 0)),
            ((0, 0, 0, 0, 0, 2, 0, 0), (0, 1, 0, 1, 0, 1, 0, 0)),
        ),
    },
    "first": (1, 2, 3, 3, 3, 4, 2, 2),
}


def frequencies():
    pair = np.arange(HEAD_SIZE // 2)
    value = np.power(1000000.0, -2.0 * pair / HEAD_SIZE).astype(np.float32)
    return np.repeat(value[:, None], HEAD_SIZE, axis=1)


def rotary_tables(places, freq):
    rows = places.shape[1]
    half = HEAD_SIZE // 2
    pair = lax.broadcasted_iota(jnp.int32, (half, rows), 0)
    first = HEAD_SIZE // 8
    second = first + 3 * HEAD_SIZE // 16
    place = places.astype(jnp.float32)
    chosen = jnp.where(pair < first, place[0:1], jnp.where(pair < second, place[1:2], place[2:3]))
    angle = chosen * jnp.concatenate([freq] * (rows // HEAD_SIZE), axis=1)
    turns = jnp.floor(angle * (2.0 / math.pi) + 0.5)
    rest = angle - turns * 1.5703125
    rest = rest - turns * 4.8351287841796875e-4
    rest = rest - turns * 3.138552419841289520264e-7
    rest = rest - turns * 6.07710050630396597660e-11
    quarter = turns.astype(jnp.int32) & 3
    square = rest * rest
    sine = rest + rest * square * (
        -1.0 / 6 + square * (1.0 / 120 + square * (-1.0 / 5040 + square * (1.0 / 362880)))
    )
    cosine = 1.0 + square * (
        -0.5 + square * (1.0 / 24 + square * (-1.0 / 720 + square * (1.0 / 40320)))
    )
    swap = (quarter & 1) == 1
    sin_turned = jnp.where(swap, cosine, sine)
    cos_turned = jnp.where(swap, sine, cosine)
    sin_turned = jnp.where(quarter >= 2, -sin_turned, sin_turned)
    cos_turned = jnp.where((quarter == 1) | (quarter == 2), -cos_turned, cos_turned)
    return cos_turned, sin_turned


def routes(blocks, lanes):
    count = blocks * lanes
    window = count // 2

    def place(r):
        return (r // lanes // 2, r % lanes), r // lanes % 2

    def member(chip, core):
        return (chip[0] * 2 + core) * lanes + chip[1]

    found = {}
    for s in range(count):
        home, own_core = place(s)
        wanting = set(range(s + 1, min(count, s + window + 1)))

        def entry(chip):
            if chip == home:
                return s
            for core in (own_core, 1 - own_core):
                if member(chip, core) in wanting:
                    return member(chip, core)
            return None

        for half in (0, 1):
            for r in sorted(wanting):
                chip, _ = place(r)
                source = entry(chip)
                if source == r:
                    options = []
                    if chip[1] != home[1]:
                        options.append(entry((chip[0], home[1])))
                    if chip[0] > home[0]:
                        options.append(entry((chip[0] - 1, chip[1])))
                    if half:
                        options.reverse()
                    options = [o for o in options if o is not None] + [s]
                    source = options[0]
                found.setdefault((source - s, r - source), (set(), set()))[half].add(source)
    return sorted(found.items(), key=lambda item: (-item[0][0], item[0][1]))


def pick(me, values):
    found = jnp.int32(values[0])
    for device, value in enumerate(values):
        if value != values[0]:
            found = jnp.where(me == device, jnp.int32(value), found)
    return found


def timetable(blocks, lanes, window):
    if (blocks, lanes) == (4, 2):
        return TABLE
    return {
        "own": {step: ((3,),) * 3 for step in range(1, blocks * lanes)},
        "relay": {slot: (((0,), (0,)),) * 2 for slot in range(1, window + 1)},
        "first": (0,),
    }


def among(me, devices):
    hit = jnp.bool_(False)
    for device in sorted(devices):
        hit = hit | (me == device)
    return hit


def kernel(
    plan, lanes, count, window, kheads,
    lengths, places_in, freq_in, keys_in, values_in, queries, out,
    places, freq, keys, values, cosine, sine, cosine_t, sine_t, kv, kfeat, qfeat, tri, qbuf, qt, scores, *rest,
):
    best, held = rest[:QUERY_PER_KEY], rest[QUERY_PER_KEY : 2 * QUERY_PER_KEY]
    q_sem, in_sem, send_sem, recv_sem = rest[2 * QUERY_PER_KEY :]
    rows = keys.shape[0]
    size = HEAD_SIZE
    group = QUERY_PER_KEY * size
    me = lax.axis_index("blk") * lanes + lax.axis_index("uly")

    def where_is(r):
        return {"blk": lax.div(r, lanes), "uly": lax.rem(r, lanes)}

    barrier = pltpu.get_barrier_semaphore()
    for offset in range(1, count):
        peer = lax.rem(me + offset, count)
        pl.semaphore_signal(
            barrier, inc=1, device_id=where_is(peer), device_id_type=pl.DeviceIdType.MESH
        )
    loads = [
        pltpu.make_async_copy(source, target, in_sem.at[i])
        for i, (source, target) in enumerate(
            ((places_in, places), (freq_in, freq), (keys_in, keys), (values_in, values))
        )
    ]
    for load in loads:
        load.start()
    fetch = pltpu.make_async_copy(queries, qbuf, q_sem)
    fetch.start()

    def column(h, width):
        return pl.ds(pl.multiple_of(h * width, width), width)

    loads[0].wait()
    loads[1].wait()
    cos_half, sin_half = rotary_tables(places[...], freq[...])
    cosine_t[...] = cos_half
    sine_t[...] = sin_half
    cosine[...] = jnp.concatenate([cos_half, cos_half], axis=0).T
    sine[...] = jnp.concatenate([-sin_half, sin_half], axis=0).T

    def turn(x):
        x = x.astype(jnp.float32)
        return (x * cosine[...] + pltpu.roll(x, size // 2, 1) * sine[...]).astype(jnp.bfloat16)

    loads[2].wait()
    loads[3].wait()

    def own_block(h, carry):
        kv[0, h, :rows, :] = turn(keys[:, column(h, size)])
        turned = values[:, column(h, size)].astype(jnp.float32).T.astype(jnp.bfloat16)
        for piece in range(rows // size):
            at = rows + piece * size
            kv[0, h, at : at + size, :] = turned[:, piece * size : (piece + 1) * size]
        return carry

    lax.fori_loop(0, kheads, own_block, 0)
    pl.semaphore_wait(barrier, count - 1)

    def copy_of(index, slot, step, h):
        return pltpu.make_async_remote_copy(
            src_ref=kv.at[slot, h],
            dst_ref=kv.at[slot + step, h],
            send_sem=send_sem.at[index, h],
            recv_sem=recv_sem.at[slot + step, h],
            device_id=where_is(me + step),
            device_id_type=pl.DeviceIdType.MESH,
        )

    def arrival(slot, h):
        return pltpu.make_async_remote_copy(
            src_ref=kv.at[slot, h],
            dst_ref=kv.at[slot, h],
            send_sem=send_sem.at[0, h],
            recv_sem=recv_sem.at[slot, h],
            device_id=where_is(me),
            device_id_type=pl.DeviceIdType.MESH,
        )

    table = timetable(count // lanes, lanes, window)
    half = kheads // 2
    quarters = (0, half, kheads * 3 // 4, kheads)

    def span(senders):
        low, high = (among(me, devices) for devices in senders)
        return jnp.where(low, 0, half), jnp.where(high, kheads, half)

    spans = [span(senders) for _, senders in plan]
    relayed = {}
    for slot in range(1, window + 1):
        ours = [senders for (from_slot, _), senders in plan if from_slot == slot]
        relayed[slot] = span([set().union(*(s[part] for s in ours)) for part in (0, 1)])

    def relays(slot, h):
        return (h >= relayed[slot][0]) & (h < relayed[slot][1])

    own_turns = []
    for index, ((slot, step), _) in enumerate(plan):
        leads = table["own"][step] if slot == 0 else ()
        edges = quarters
        if len(set(leads)) == 1:
            leads, edges = leads[:1], (0, kheads)
        for part, lead in enumerate(leads):
            ahead = pick(me, lead)
            start = jnp.maximum(spans[index][0], edges[part]) - ahead
            stop = jnp.minimum(spans[index][1], edges[part + 1]) - ahead
            own_turns.append((index, step, ahead, start, stop))

    relay_turns = []
    for slot in sorted({slot for (slot, _), _ in plan if slot}, reverse=True):
        turns, edges = table["relay"][slot], (0, half, kheads)
        if len(set(turns)) == 1:
            turns, edges = turns[:1], (0, kheads)
        for part, (lead, at) in enumerate(turns):
            ahead, where = pick(me, lead), pick(me, at)
            start = jnp.maximum(relayed[slot][0], edges[part]) - ahead
            stop = jnp.minimum(relayed[slot][1], edges[part + 1]) - ahead
            for place in sorted(set(at)):
                stop_here = jnp.where(where == place, stop, start)
                relay_turns.append((place, slot, ahead, start, stop_here))

    def due(turn_at, turns):
        hit = jnp.bool_(False)
        for *_, start, stop in turns:
            hit = hit | ((turn_at >= start) & (turn_at < stop))
        return hit

    def send_own(turn_at):
        @pl.when(due(turn_at, own_turns))
        def _():
            for index, step, ahead, start, stop in own_turns:
                @pl.when((turn_at >= start) & (turn_at < stop))
                def _():
                    copy_of(index, 0, step, turn_at + ahead).start()

    def pass_on(turn_at, place):
        turns = [turn[1:] for turn in relay_turns if turn[0] == place]

        @pl.when(due(turn_at, turns))
        def _():
            for slot, ahead, start, stop in turns:
                @pl.when((turn_at >= start) & (turn_at < stop))
                def _():
                    h = turn_at + ahead
                    arrival(slot, h).wait_recv()
                    for index, ((from_slot, step), _) in enumerate(plan):
                        if from_slot == slot:
                            @pl.when((h >= spans[index][0]) & (h < spans[index][1]))
                            def _():
                                copy_of(index, slot, step, h).start()

    def opening(i, carry):
        turn_at = i - BURST
        send_own(turn_at)
        for place in range(3):
            pass_on(turn_at, place)
        return carry

    lax.fori_loop(0, BURST - SETTLED, opening, 0)

    for slot in range(1, window + 1):
        @pl.when(me < slot)
        def _():
            def clear(h, carry):
                kv[slot, h] = jnp.zeros((rows + rows // size * size, size), kv.dtype)
                return carry

            lax.fori_loop(0, kheads, clear, 0)

    lane = lax.broadcasted_iota(jnp.int32, (1, size), 1)
    opens = jnp.zeros((1, size), jnp.int32)
    closes = jnp.zeros((1, size), jnp.int32)
    end = jnp.int32(0)
    for d in range(lengths.shape[0]):
        start, end = end, end + lengths[d]
        opens = jnp.where(lane == d, start, opens)
        closes = jnp.where(lane == d, end, closes)
    row = lax.broadcasted_iota(jnp.int32, (rows, size), 0)
    for slot in range(window + 1):
        token = row + (me - slot) * rows
        inside = (token >= opens) & (token < closes)
        kfeat[slot] = jnp.where(inside, 0.0, FAR).astype(jnp.bfloat16)
        if slot == 0:
            qfeat[...] = jnp.where(inside, 1.0, 0.0).T.astype(jnp.bfloat16)
    key_at = lax.broadcasted_iota(jnp.int32, (rows, rows), 0)
    query_at = lax.broadcasted_iota(jnp.int32, (rows, rows), 1)
    tri[...] = jnp.where(key_at <= query_at, 1.0, 0.0).astype(jnp.bfloat16)

    fetch.wait()

    def turn_queries(h, carry):
        cos_half, sin_half = cosine_t[...], sine_t[...]
        x = qbuf[:, column(h, group)].T
        for g in range(QUERY_PER_KEY):
            low = x[g * size : g * size + size // 2].astype(jnp.float32)
            high = x[g * size + size // 2 : (g + 1) * size].astype(jnp.float32)
            turned = jnp.concatenate(
                [low * cos_half - high * sin_half, high * cos_half + low * sin_half], axis=0
            )
            qt[h * QUERY_PER_KEY + g] = turned.astype(jnp.bfloat16)
        return carry

    lax.fori_loop(0, kheads, turn_queries, 0)

    scale = math.log2(math.e) / math.sqrt(size)
    ones = jnp.ones((2 * SUBLANES, rows), jnp.bfloat16)

    def key_of(slot, h):
        return jnp.concatenate([kv[slot, h, :rows, :], kfeat[slot]], axis=1)

    def value_of(slot, h):
        pieces = [
            kv[slot, h, rows + p * size : rows + (p + 1) * size, :] for p in range(rows // size)
        ]
        return jnp.concatenate([jnp.concatenate(pieces, axis=1), ones], axis=0)

    def query_of(h, g):
        return jnp.concatenate([qt[h * QUERY_PER_KEY + g], qfeat[...]], axis=0)

    def dot(a, b):
        return jnp.dot(a, b, preferred_element_type=jnp.float32)

    def begin(h):
        scores = []
        for g in range(QUERY_PER_KEY):
            q = query_of(h, g)
            scores.append(
                jnp.where(key_at <= query_at, dot(key_of(0, h), q), dot(key_of(window, h), q))
            )
        pending = None
        for g in range(QUERY_PER_KEY + 1):
            if g < QUERY_PER_KEY:
                top = jnp.max(scores[g], axis=0, keepdims=True)
                w = jnp.exp2((scores[g] - top) * scale).astype(jnp.bfloat16)
                near = w * tri[...]
                best[g][h] = jnp.broadcast_to(top, (SUBLANES, rows))
                both = dot(value_of(0, h), near) + dot(value_of(window, h), w - near)
            if pending is not None:
                held[g - 1][h] = pending[: size + SUBLANES]
            pending = both

    def complete(h):
        def score(g):
            q = query_of(h, g)
            top = best[g][h][:1]
            for slot in range(1, window):
                s = dot(key_of(slot, h), q)
                scores[g, slot - 1] = s
                top = jnp.maximum(top, jnp.max(s, axis=0, keepdims=True))
            return top

        def attend(g, top):
            keep = jnp.exp2((best[g][h][:1] - top) * scale)
            both = None
            for slot in range(1, window):
                w = jnp.exp2((scores[g, slot - 1] - top) * scale).astype(jnp.bfloat16)
                part = dot(value_of(slot, h), w)
                both = part if both is None else both + part
            return both[: size + SUBLANES] + held[g][h] * keep

        tops = [score(g) for g in range(SCORES_FIRST)]
        pending = None
        for g in range(QUERY_PER_KEY):
            if g + SCORES_FIRST < QUERY_PER_KEY:
                tops.append(score(g + SCORES_FIRST))
            both = attend(g, tops[g])
            if pending is not None:
                settle(h, g - 1, pending)
            pending = both
        settle(h, QUERY_PER_KEY - 1, pending)

    def settle(h, g, both):
        result = both[:size] * (1.0 / both[size : size + 1])
        at = pl.ds(pl.multiple_of(h * group + g * size, size), size)
        out[:, at] = result.T.astype(jnp.bfloat16)

    def take(slot, h):
        @pl.when((me >= slot) & jnp.logical_not(relays(slot, h)))
        def _():
            arrival(slot, h).wait_recv()

    def rounds(i, carry):
        turn_at = i - SETTLED
        send_own(turn_at)
        pass_on(turn_at, 0)
        first = turn_at + pick(me, table["first"])

        @pl.when((first >= 0) & (first < kheads))
        def _():
            take(window, first)
            begin(first)

        pass_on(turn_at, 1)

        @pl.when(turn_at >= 0)
        def _():
            for slot in range(1, window):
                take(slot, turn_at)

            complete(turn_at)

        pass_on(turn_at, 2)
        return carry

    lax.fori_loop(0, SETTLED + kheads, rounds, 0)

    for index, ((slot, step), _) in enumerate(plan):
        def finish(h, carry):
            copy_of(index, slot, step, h).wait_send()
            return carry

        lax.fori_loop(spans[index][0], spans[index][1], finish, 0)


def local(blocks, lanes, queries, keys, values, positions, doc_lengths):
    rows = queries.shape[0]
    kheads = keys.shape[1] // HEAD_SIZE
    count = blocks * lanes
    window = count // 2
    plan = routes(blocks, lanes)
    vmem = pl.BlockSpec(memory_space=pltpu.VMEM)
    anywhere = pl.BlockSpec(memory_space=pl.ANY)
    freq = jnp.asarray(frequencies())
    return pl.pallas_call(
        functools.partial(kernel, plan, lanes, count, window, kheads),
        out_shape=pltpu.VMEM(queries.shape, jnp.bfloat16),
        in_specs=[pl.BlockSpec(memory_space=pltpu.SMEM)] + [anywhere] * 5,
        out_specs=vmem,
        scratch_shapes=[
            pltpu.VMEM(positions.shape, jnp.int32),
            pltpu.VMEM(freq.shape, jnp.float32),
            pltpu.VMEM(keys.shape, jnp.bfloat16),
            pltpu.VMEM(values.shape, jnp.bfloat16),
            pltpu.VMEM((rows, HEAD_SIZE), jnp.float32),
            pltpu.VMEM((rows, HEAD_SIZE), jnp.float32),
            pltpu.VMEM((HEAD_SIZE // 2, rows), jnp.float32),
            pltpu.VMEM((HEAD_SIZE // 2, rows), jnp.float32),
            pltpu.VMEM((window + 1, kheads, 2 * rows, HEAD_SIZE), jnp.bfloat16),
            pltpu.VMEM((window + 1, rows, HEAD_SIZE), jnp.bfloat16),
            pltpu.VMEM((HEAD_SIZE, rows), jnp.bfloat16),
            pltpu.VMEM((rows, rows), jnp.bfloat16),
            pltpu.VMEM(queries.shape, jnp.bfloat16),
            pltpu.VMEM((kheads * QUERY_PER_KEY, HEAD_SIZE, rows), jnp.bfloat16),
            pltpu.VMEM((QUERY_PER_KEY, window - 1, rows, rows), jnp.float32),
            *[pltpu.VMEM((kheads, SUBLANES, rows), jnp.float32)] * QUERY_PER_KEY,
            *[pltpu.VMEM((kheads, HEAD_SIZE + SUBLANES, rows), jnp.float32)] * QUERY_PER_KEY,
            pltpu.SemaphoreType.DMA,
            pltpu.SemaphoreType.DMA((4,)),
            pltpu.SemaphoreType.DMA((len(plan), kheads)),
            pltpu.SemaphoreType.DMA((window + 1, kheads)),
        ],
        compiler_params=pltpu.CompilerParams(
            collective_id=0, has_side_effects=True, vmem_limit_bytes=60 * 1024 * 1024
        ),
        name="windowed_attention",
    )(doc_lengths, positions, freq, keys, values, queries)


def solution(mesh):
    in_specs = (
        P(("seq", "blk", "uly"), None),
        P(("seq", "blk", "uly"), None),
        P(("seq", "blk", "uly"), None),
        P(None, ("seq", "blk", "uly")),
        P("seq"),
    )
    out_specs = P(("seq", "blk", "uly"), None)
    body = functools.partial(local, mesh.shape["blk"], mesh.shape["uly"])
    return jax.shard_map(body, mesh=mesh, in_specs=in_specs, out_specs=out_specs, check_vma=False)
```
